32 devices in a mesh: band: 8 (over y, x, core), pw: 4 (over z).
Axes of the slice: x: 2, y: 2, z: 4, core: 2. Of those that a mesh axis runs over, the one named last changes fastest.
Arguments:
- pair_density: bfloat16 [40, 128, 9216], P('band', None, 'pw'), may hold values from -6 to 6
- eigvecs: bfloat16 [2944, 9216], P('band', 'pw'), may hold values from -0.0625 to 0.0625
- screening: bfloat16 [2944, 2944], P('pw'), may hold values from -0.00048828125 to 0.00048828125
- occupation: float32 [16], replicated, may hold values from 0 to 1
- window_start: int32 [40], P('band'), may hold values from 0 to 511, as said below
- window_len: int32 [40], P('band'), may hold values from 1 to 128, as said below
- slot_band: int32 [40], P('band'), may hold values from -1 to 15, as said below
Outputs:
- sigma: float32 [512, 512], P(('band', 'pw'))
The draws below stay inside these ranges and needn't reach their ends.
Inputs may be any that keep to these rules, and one draw needn't show every extreme that they name: window_start + window_len <= 512 for every slot. `window_len`: some slot has a window of 128 bands. On each index of band the live slots (slot_band >= 0) come first among its 5 slots; each index holds 3 to 5 live slots, and the counts of index i and index i + 8 / 2 add up to 8.
All inputs are finite; a program needn't handle non-finite values.
Results may differ from the reference program's by a relative error of at most 0.0049.
Values may be sent and summed in bfloat16 or wider, within the bound.
A program may use at most 128 MiB of HBM per device.

```python
import jax
import jax.numpy as jnp
from jax import lax

NB_SIGMA = 512
BLOCK = 128
G = 9216
S = 2944
CAP = 5
SLOTS = 40
NSUM = 16


def window_parts(key):
    lengths = jax.random.randint(jax.random.fold_in(key, 11), (SLOTS,), 1, BLOCK + 1)
    lengths = lengths.at[0].set(BLOCK)
    lengths = lengths.at[1].set(1)
    spaces = NB_SIGMA - lengths + 1
    raw_bits = jax.random.randint(jax.random.fold_in(key, 12), (SLOTS,), 0, 1 << 30)
    starts = raw_bits % spaces
    starts = starts.at[0].set(0)
    starts = starts.at[1].set(NB_SIGMA - 1)
    return (starts.astype(jnp.int32), lengths.astype(jnp.int32))


def draw_window_start(key, part):
    starts, lengths = window_parts(key)
    return starts


def draw_window_len(key, part):
    starts, lengths = window_parts(key)
    return lengths


def draw_slot_band(key, part):
    groups = SLOTS // CAP
    halves = groups // 2
    lower = jax.random.randint(jax.random.fold_in(key, 21), (halves,), CAP - 2, CAP + 1)
    counts = jnp.concatenate([lower, 2 * CAP - 2 - lower])
    position = jnp.arange(SLOTS, dtype=jnp.int32) % CAP
    device = jnp.arange(SLOTS, dtype=jnp.int32) // CAP
    band_ids = jax.random.randint(jax.random.fold_in(key, 22), (SLOTS,), 0, NSUM)
    return jnp.where(position < counts[device], band_ids, -1).astype(jnp.int32)


def steps_of(own_key, extent, pieces, least, top_value):
    def one(axis_at, parts):
        heights = jax.random.uniform(jax.random.fold_in(jax.random.fold_in(own_key, 6), axis_at), (parts,), jnp.float32, least / len(pieces), top_value / len(pieces))
        return jnp.repeat(jnp.exp(heights), extent[axis_at] // parts).reshape((-1,) + (1,) * (len(extent) - axis_at - 1))

    level = one(*pieces[0])
    for cut in pieces[1:]:
        level = level * one(*cut)
    return level


def noise(own_key, shape, width, bound, pieces=(), kind=jnp.bfloat16):
    result = jax.random.normal(own_key, shape, jnp.float32) * width
    if len(pieces) > 0:
        result = steps_of(own_key, shape, pieces, -0.22, 0.18) * result
    return jnp.clip(result, min=-bound, max=bound).astype(kind)


def setup_inputs(seed: int = 0) -> dict:
    streams_of = jax.random.split(jax.random.key(seed), 8)
    return {
        "pair_density": noise(streams_of[0], (SLOTS, BLOCK, G), 1.0, 6.0, ((0, 8), (2, 4))),
        "eigvecs": noise(streams_of[1], (S, G), G ** -0.5, 0.0625, ((0, 8), (1, 4))),
        "screening": noise(streams_of[2], (S, S), (16 * S * S) ** -0.5, 0.00048828125, ((0, 4),)),
        "occupation": jnp.clip(jax.random.uniform(streams_of[3], (NSUM,), jnp.float32, 0.0, 1.0), 0.0, 1.0),
        "window_start": draw_window_start(jax.random.fold_in(streams_of[7], 71), 0),
        "window_len": draw_window_len(jax.random.fold_in(streams_of[7], 71), 0),
        "slot_band": draw_slot_band(jax.random.fold_in(streams_of[7], 71), 0),
    }


def reference(pair_density, eigvecs, screening, occupation, window_start, window_len, slot_band):
    row_ids = jnp.arange(BLOCK, dtype=jnp.int32)
    band_list = jnp.arange(NSUM, dtype=jnp.int32)

    def add_slot(totals, item):
        density, offset, length, band_id = item
        raw_proj = jnp.dot(density, eigvecs.T, preferred_element_type=jnp.float32)
        keep_rows = ((row_ids < length) & (band_id >= 0)).astype(jnp.float32)
        projected = (raw_proj * keep_rows[:, None]).astype(jnp.bfloat16)
        screened = jnp.dot(projected, screening.T, preferred_element_type=jnp.float32).astype(jnp.bfloat16)
        block_sigma = jnp.dot(screened, projected.T, preferred_element_type=jnp.float32)
        weight = 0.5 - jnp.sum(jnp.where(band_list == band_id, occupation, jnp.zeros_like(occupation)))
        first = offset.astype(jnp.int32)
        previous = lax.dynamic_slice(totals, (first, first), (BLOCK, BLOCK))
        totals = lax.dynamic_update_slice(totals, previous + weight * block_sigma, (first, first))
        return totals, None

    start_sum = jnp.zeros((NB_SIGMA + BLOCK, NB_SIGMA + BLOCK), jnp.float32)
    totals, unused = lax.scan(add_slot, start_sum, (pair_density, window_start, window_len, slot_band))
    return totals[:NB_SIGMA, :NB_SIGMA]
```

```python
import functools

import jax
import jax.numpy as jnp
from jax import lax
from jax.experimental import pallas as pl
from jax.experimental.pallas import tpu as pltpu
from jax.sharding import PartitionSpec as P

NB_SIGMA = 512


def ring_per_device(pair_density, eigvecs, screening, occupation, window_start, window_len, slot_band):
    capacity, block, plane_rows = pair_density.shape
    density, starts, lengths, band_ids = (pair_density, window_start, window_len, slot_band)
    slots = density.shape[0]
    flat = density.reshape(slots * block, plane_rows)
    partial_proj = lax.dot_general(
        flat,
        lax.all_gather(eigvecs, "band", axis=0, tiled=True),
        (((1,), (1,)), ((), ())),
        preferred_element_type=jnp.float32,
    )
    row_ids = jnp.arange(block, dtype=jnp.int32)
    keep_rows = ((row_ids[None, :] < lengths[:, None]) & (band_ids[:, None] >= 0)).astype(
        jnp.float32
    )
    masked = partial_proj * keep_rows.reshape(slots * block, 1)
    projected = lax.psum(masked, "pw").astype(jnp.bfloat16)
    width = screening.shape[0]
    own_cols = lax.dynamic_slice_in_dim(projected, lax.axis_index("pw") * width, width, 1)
    screened = lax.dot_general(
        projected, screening, (((1,), (1,)), ((), ())), preferred_element_type=jnp.float32
    ).astype(jnp.bfloat16)
    block_sigma = lax.dot_general(
        screened.reshape(slots, block, width),
        own_cols.reshape(slots, block, width),
        (((2,), (2,)), ((0,), (0,))),
        preferred_element_type=jnp.float32,
    )
    band_list = jnp.arange(occupation.shape[0], dtype=jnp.int32)
    weights = 0.5 - jnp.sum(
        jnp.where(band_list[None, :] == band_ids[:, None], occupation[None, :], 0.0), axis=1
    )
    totals = jnp.zeros((NB_SIGMA + block, NB_SIGMA + block), jnp.float32)
    for index in range(slots):
        first = starts[index]
        previous = lax.dynamic_slice(totals, (first, first), (block, block))
        totals = lax.dynamic_update_slice(
            totals, previous + weights[index] * block_sigma[index], (first, first)
        )
    sigma_part = totals[:NB_SIGMA, :NB_SIGMA]
    by_band = lax.psum_scatter(sigma_part, "band", scatter_dimension=0, tiled=True)
    return lax.psum_scatter(by_band, "pw", scatter_dimension=0, tiled=True)


def flip(index, relation):
    total = 0
    for place in (4, 2, 1):
        bit = lax.rem(index // place, 2)
        other = lax.rem(relation // place, 2)
        total = total + place * (bit + other - 2 * bit * other)
    return total


def fused_kernel(
    density_ref, eig_ref, screen_ref, keep_ref, weight_ref, out_ref,
    eig, screen, part, sent, own, landed, proj, acc,
    load_sem, eig_send, eig_recv, red_send, red_recv, up_send, up_recv, down_send, down_recv,
):
    mesh_id = pl.DeviceIdType.MESH
    band, z = lax.axis_index("band"), lax.axis_index("pw")
    n_rel, depth, _ = eig.shape
    n_z = landed.shape[1] + 1
    rows = own.shape[1]
    slots, block, _ = out_ref.shape

    barrier = pltpu.get_barrier_semaphore()
    for rel in (1, 2, 4, 6):
        pl.semaphore_signal(barrier, inc=1, device_id=(flip(band, rel), z), device_id_type=mesh_id)
    for k in range(1, n_z):
        pl.semaphore_signal(
            barrier, inc=1, device_id=(band, lax.rem(z + k, n_z)), device_id_type=mesh_id
        )
    load = pltpu.make_async_copy(eig_ref, eig.at[0], load_sem)
    load.start()
    pl.semaphore_wait(barrier, 4 + n_z - 1)

    def eig_copy(rel):
        return pltpu.make_async_remote_copy(
            src_ref=eig_ref, dst_ref=eig.at[rel], send_sem=eig_send.at[rel],
            recv_sem=eig_recv.at[rel], device_id=(flip(band, rel), z), device_id_type=mesh_id,
        )

    def forward_copy(rel):
        return pltpu.make_async_remote_copy(
            src_ref=eig.at[rel], dst_ref=eig.at[rel + 1], send_sem=eig_send.at[rel + 1],
            recv_sem=eig_recv.at[rel + 1], device_id=(flip(band, 1), z), device_id_type=mesh_id,
        )

    for rel in (1, 2, 4, 6):
        eig_copy(rel).start()
    for index in range(n_rel):
        screen[index] = screen_ref[:, index * depth : (index + 1) * depth]
    acc[...] = jnp.zeros_like(acc)
    load.wait()

    def red_copy(rel, k):
        target = lax.rem(z + k, n_z)
        return pltpu.make_async_remote_copy(
            src_ref=sent.at[rel, target], dst_ref=landed.at[rel, k - 1],
            send_sem=red_send.at[rel, k - 1], recv_sem=red_recv.at[rel, k - 1],
            device_id=(band, target), device_id_type=mesh_id,
        )

    def up_copy(rel, hop):
        source = lax.rem(z - hop + n_z, n_z)
        return pltpu.make_async_remote_copy(
            src_ref=proj.at[rel, source], dst_ref=proj.at[rel, source],
            send_sem=up_send.at[rel, hop], recv_sem=up_recv.at[rel, hop],
            device_id=(band, lax.rem(z + 1, n_z)), device_id_type=mesh_id,
        )

    def down_copy(rel, hop):
        source = lax.rem(z + hop, n_z)
        return pltpu.make_async_remote_copy(
            src_ref=proj.at[rel, source], dst_ref=proj.at[rel, source],
            send_sem=down_send.at[rel, hop], recv_sem=down_recv.at[rel, hop],
            device_id=(band, lax.rem(z + n_z - 1, n_z)), device_id_type=mesh_id,
        )

    def landing(rel, hop, up):
        source = lax.rem(z - hop - 1 + 2 * n_z, n_z) if up else lax.rem(z + hop + 1, n_z)
        return pltpu.make_async_remote_copy(
            src_ref=proj.at[rel, source], dst_ref=proj.at[rel, source],
            send_sem=(up_send if up else down_send).at[rel, hop],
            recv_sem=(up_recv if up else down_recv).at[rel, hop],
            device_id=(band, lax.rem(z + 1, n_z)), device_id_type=mesh_id,
        )

    def pass_on(rel, hop):
        @pl.when((z - hop >= 0) & (z + 1 < n_z))
        def _():
            up_copy(rel, hop).start()

        @pl.when((z + hop < n_z) & (z >= 1))
        def _():
            down_copy(rel, hop).start()

    def take(rel, hop):
        @pl.when(z - hop - 1 >= 0)
        def _():
            landing(rel, hop, True).wait_recv()

        @pl.when(z + hop + 1 < n_z)
        def _():
            landing(rel, hop, False).wait_recv()

    def project(rel):
        @pl.when(rel >= 1)
        def _():
            eig_copy(rel).wait_recv()

        @pl.when((rel >= 2) & (lax.rem(rel, 2) == 0))
        def _():
            forward_copy(rel).start()

        part[...] = lax.dot_general(
            density_ref[...], eig[rel], (((1,), (1,)), ((), ())),
            preferred_element_type=jnp.float32,
        ).reshape(part.shape)
        sent[rel] = part[...].astype(jnp.bfloat16)
        own[rel] = part[z]
        for k in (2, 1, 3):
            red_copy(rel, k).start()

    def reduce(rel):
        for k in range(1, n_z):
            red_copy(rel, k).wait_recv()
        total = own[rel]
        for k in range(1, n_z):
            total = total + landed[rel, k - 1].astype(jnp.float32)
        proj[rel, z] = (total * keep_ref[z]).astype(jnp.bfloat16)
        pass_on(rel, 0)

    def screen_step(rel):
        take(rel, n_z - 2)
        whole = proj[rel].reshape(n_z * rows, depth)
        at = flip(band, rel)
        for half in range(2):
            acc[half] += lax.dot_general(
                whole, screen[at, half * depth : (half + 1) * depth], (((1,), (1,)), ((), ())),
                preferred_element_type=jnp.float32,
            )

    def step(t, carry):
        @pl.when(t < n_rel)
        def _():
            project(t)

        @pl.when((t >= 1) & (t < n_rel + 1))
        def _():
            reduce(t - 1)

        for hop in range(n_z - 2):
            @pl.when((t >= 2 + hop) & (t < n_rel + 2 + hop))
            def _():
                take(t - 2 - hop, hop)
                pass_on(t - 2 - hop, hop + 1)

        @pl.when(t >= n_z)
        def _():
            screen_step(t - n_z)

        return carry

    lax.fori_loop(0, n_rel + n_z, step, 0)

    screened = acc[...].astype(jnp.bfloat16)
    pairs = [proj[flip(band, 2 * z + half)].reshape(n_z * rows, depth) for half in range(2)]
    for slot in range(slots):
        here = slice(slot * block, (slot + 1) * block)
        total = 0.0
        for half in range(2):
            total = total + lax.dot_general(
                screened[half, here], pairs[half][here], (((1,), (1,)), ((), ())),
                preferred_element_type=jnp.float32,
            )
        out_ref[slot] = total * weight_ref[slot]

    for rel in (1, 2, 4, 6):
        eig_copy(rel).wait_send()
    for rel in (2, 4, 6):
        forward_copy(rel).wait_send()

    def drain(rel, carry):
        for k in range(1, n_z):
            red_copy(rel, k).wait_send()
        for hop in range(n_z - 1):
            @pl.when((z - hop >= 0) & (z + 1 < n_z))
            def _():
                up_copy(rel, hop).wait_send()

            @pl.when((z + hop < n_z) & (z >= 1))
            def _():
                down_copy(rel, hop).wait_send()
        return carry

    lax.fori_loop(0, n_rel, drain, 0)


def per_device(
    n_z, n_rel, pair_density, eigvecs, screening, occupation, window_start, window_len, slot_band
):
    slots, block, plane_rows = pair_density.shape
    depth, width = eigvecs.shape[0], screening.shape[0]
    rows = slots * block // n_z
    keep_rows = (
        (jnp.arange(block, dtype=jnp.int32)[None, :] < window_len[:, None])
        & (slot_band[:, None] >= 0)
    ).astype(jnp.float32)
    band_list = jnp.arange(occupation.shape[0], dtype=jnp.int32)
    weights = 0.5 - jnp.sum(
        jnp.where(band_list[None, :] == slot_band[:, None], occupation[None, :], 0.0), axis=1
    )
    dma = pltpu.SemaphoreType.DMA
    vmem = pl.BlockSpec(memory_space=pltpu.VMEM)
    block_sigma = pl.pallas_call(
        fused_kernel,
        out_shape=jax.ShapeDtypeStruct((slots, block, block), jnp.float32),
        in_specs=[vmem, pl.BlockSpec(memory_space=pl.ANY), vmem, vmem, vmem],
        out_specs=vmem,
        scratch_shapes=[
            pltpu.VMEM((n_rel, depth, plane_rows), jnp.bfloat16),
            pltpu.VMEM((n_rel, width, depth), jnp.bfloat16),
            pltpu.VMEM((n_z, rows, depth), jnp.float32),
            pltpu.VMEM((n_rel, n_z, rows, depth), jnp.bfloat16),
            pltpu.VMEM((n_rel, rows, depth), jnp.float32),
            pltpu.VMEM((n_rel, n_z - 1, rows, depth), jnp.bfloat16),
            pltpu.VMEM((n_rel, n_z, rows, depth), jnp.bfloat16),
            pltpu.VMEM((2, slots * block, depth), jnp.float32),
            dma,
            dma((n_rel,)),
            dma((n_rel,)),
            dma((n_rel, n_z - 1)),
            dma((n_rel, n_z - 1)),
            dma((n_rel, n_z - 1)),
            dma((n_rel, n_z - 1)),
            dma((n_rel, n_z - 1)),
            dma((n_rel, n_z - 1)),
        ],
        compiler_params=pltpu.CompilerParams(
            collective_id=0, has_side_effects=True, vmem_limit_bytes=60 * 2**20
        ),
    )(
        pair_density.reshape(slots * block, plane_rows),
        eigvecs,
        screening,
        keep_rows.reshape(n_z, rows, 1),
        jnp.broadcast_to(weights[:, None, None], (slots, 8, block))[:, :1],
    )
    return finish(block_sigma, window_start)


def finish(block_sigma, window_start):
    slots, block, _ = block_sigma.shape
    totals = jnp.zeros((NB_SIGMA + block, NB_SIGMA + block), jnp.float32)
    for index in range(slots):
        first = window_start[index]
        previous = lax.dynamic_slice(totals, (first, first), (block, block))
        totals = lax.dynamic_update_slice(totals, previous + block_sigma[index], (first, first))
    sigma_part = totals[:NB_SIGMA, :NB_SIGMA]
    by_band = lax.psum_scatter(sigma_part, "band", scatter_dimension=0, tiled=True)
    return lax.psum_scatter(by_band, "pw", scatter_dimension=0, tiled=True)


def solution(mesh):
    n_band, n_z = mesh.shape["band"], mesh.shape["pw"]
    body = ring_per_device
    if n_band == 8 and n_z == 4:
        body = functools.partial(per_device, n_z, n_band)
    return jax.shard_map(
        body,
        mesh=mesh,
        in_specs=(
            P("band", None, "pw"),
            P("band", "pw"),
            P("pw", None),
            P(),
            P("band"),
            P("band"),
            P("band"),
        ),
        out_specs=P(("band", "pw"), None),
        check_vma=False,
    )
```

```python
import functools

import jax
import jax.numpy as jnp
from jax import lax
from jax.experimental import pallas as pl
from jax.experimental.pallas import tpu as pltpu
from jax.sharding import PartitionSpec as P

NB_SIGMA = 512


def ring_per_device(pair_density, eigvecs, screening, occupation, window_start, window_len, slot_band):
    capacity, block, plane_rows = pair_density.shape
    density, starts, lengths, band_ids = (pair_density, window_start, window_len, slot_band)
    slots = density.shape[0]
    flat = density.reshape(slots * block, plane_rows)
    partial_proj = lax.dot_general(
        flat,
        lax.all_gather(eigvecs, "band", axis=0, tiled=True),
        (((1,), (1,)), ((), ())),
        preferred_element_type=jnp.float32,
    )
    row_ids = jnp.arange(block, dtype=jnp.int32)
    keep_rows = ((row_ids[None, :] < lengths[:, None]) & (band_ids[:, None] >= 0)).astype(
        jnp.float32
    )
    masked = partial_proj * keep_rows.reshape(slots * block, 1)
    projected = lax.psum(masked, "pw").astype(jnp.bfloat16)
    width = screening.shape[0]
    own_cols = lax.dynamic_slice_in_dim(projected, lax.axis_index("pw") * width, width, 1)
    screened = lax.dot_general(
        projected, screening, (((1,), (1,)), ((), ())), preferred_element_type=jnp.float32
    ).astype(jnp.bfloat16)
    block_sigma = lax.dot_general(
        screened.reshape(slots, block, width),
        own_cols.reshape(slots, block, width),
        (((2,), (2,)), ((0,), (0,))),
        preferred_element_type=jnp.float32,
    )
    band_list = jnp.arange(occupation.shape[0], dtype=jnp.int32)
    weights = 0.5 - jnp.sum(
        jnp.where(band_list[None, :] == band_ids[:, None], occupation[None, :], 0.0), axis=1
    )
    totals = jnp.zeros((NB_SIGMA + block, NB_SIGMA + block), jnp.float32)
    for index in range(slots):
        first = starts[index]
        previous = lax.dynamic_slice(totals, (first, first), (block, block))
        totals = lax.dynamic_update_slice(
            totals, previous + weights[index] * block_sigma[index], (first, first)
        )
    sigma_part = totals[:NB_SIGMA, :NB_SIGMA]
    by_band = lax.psum_scatter(sigma_part, "band", scatter_dimension=0, tiled=True)
    return lax.psum_scatter(by_band, "pw", scatter_dimension=0, tiled=True)


def flip(index, relation):
    total = 0
    for place in (4, 2, 1):
        bit = lax.rem(index // place, 2)
        other = lax.rem(relation // place, 2)
        total = total + place * (bit + other - 2 * bit * other)
    return total


def split(value):
    top = value.astype(jnp.bfloat16)
    return top, (value - top.astype(jnp.float32)).astype(jnp.bfloat16)


def fused_kernel(
    density_ref, eig_ref, screen_ref, keep_ref, weight_ref, start_ref, out_ref,
    eig, screen, part, sent, own, landed, proj, acc,
    place, high, low, sigma, band_sum, sigma_in, band_in,
    load_sem, eig_send, eig_recv, red_send, red_recv, up_send, up_recv, down_send, down_recv,
    sig_send, sig_recv, fin_send, fin_recv,
):
    mesh_id = pl.DeviceIdType.MESH
    band, z = lax.axis_index("band"), lax.axis_index("pw")
    n_rel, depth, _ = eig.shape
    n_z = landed.shape[1] + 1
    rows = own.shape[1]
    slots, block = weight_ref.shape[0], weight_ref.shape[2]

    barrier = pltpu.get_barrier_semaphore()
    for rel in range(1, n_rel):
        pl.semaphore_signal(barrier, inc=1, device_id=(flip(band, rel), z), device_id_type=mesh_id)
    for k in range(1, n_z):
        pl.semaphore_signal(
            barrier, inc=1, device_id=(band, lax.rem(z + k, n_z)), device_id_type=mesh_id
        )
    load = pltpu.make_async_copy(eig_ref, eig.at[0], load_sem)
    load.start()
    pl.semaphore_wait(barrier, n_rel - 1 + n_z - 1)

    def eig_copy(rel):
        return pltpu.make_async_remote_copy(
            src_ref=eig_ref, dst_ref=eig.at[rel], send_sem=eig_send.at[rel],
            recv_sem=eig_recv.at[rel], device_id=(flip(band, rel), z), device_id_type=mesh_id,
        )

    def forward_copy(rel):
        return pltpu.make_async_remote_copy(
            src_ref=eig.at[rel], dst_ref=eig.at[rel + 1], send_sem=eig_send.at[rel + 1],
            recv_sem=eig_recv.at[rel + 1], device_id=(flip(band, 1), z), device_id_type=mesh_id,
        )

    for rel in (1, 2, 4, 6):
        eig_copy(rel).start()
    for index in range(n_rel):
        screen[index] = screen_ref[:, index * depth : (index + 1) * depth]
    acc[...] = jnp.zeros_like(acc)
    load.wait()

    def red_copy(rel, k):
        target = lax.rem(z + k, n_z)
        return pltpu.make_async_remote_copy(
            src_ref=sent.at[rel, target], dst_ref=landed.at[rel, k - 1],
            send_sem=red_send.at[rel, k - 1], recv_sem=red_recv.at[rel, k - 1],
            device_id=(band, target), device_id_type=mesh_id,
        )

    def up_copy(rel, hop):
        source = lax.rem(z - hop + n_z, n_z)
        return pltpu.make_async_remote_copy(
            src_ref=proj.at[rel, source], dst_ref=proj.at[rel, source],
            send_sem=up_send.at[rel, hop], recv_sem=up_recv.at[rel, hop],
            device_id=(band, lax.rem(z + 1, n_z)), device_id_type=mesh_id,
        )

    def down_copy(rel, hop):
        source = lax.rem(z + hop, n_z)
        return pltpu.make_async_remote_copy(
            src_ref=proj.at[rel, source], dst_ref=proj.at[rel, source],
            send_sem=down_send.at[rel, hop], recv_sem=down_recv.at[rel, hop],
            device_id=(band, lax.rem(z + n_z - 1, n_z)), device_id_type=mesh_id,
        )

    def landing(rel, hop, up):
        source = lax.rem(z - hop - 1 + 2 * n_z, n_z) if up else lax.rem(z + hop + 1, n_z)
        return pltpu.make_async_remote_copy(
            src_ref=proj.at[rel, source], dst_ref=proj.at[rel, source],
            send_sem=(up_send if up else down_send).at[rel, hop],
            recv_sem=(up_recv if up else down_recv).at[rel, hop],
            device_id=(band, lax.rem(z + 1, n_z)), device_id_type=mesh_id,
        )

    def pass_on(rel, hop):
        @pl.when((z - hop >= 0) & (z + 1 < n_z))
        def _():
            up_copy(rel, hop).start()

        @pl.when((z + hop < n_z) & (z >= 1))
        def _():
            down_copy(rel, hop).start()

    def take(rel, hop):
        @pl.when(z - hop - 1 >= 0)
        def _():
            landing(rel, hop, True).wait_recv()

        @pl.when(z + hop + 1 < n_z)
        def _():
            landing(rel, hop, False).wait_recv()

    def project(rel):
        @pl.when(rel >= 1)
        def _():
            eig_copy(rel).wait_recv()

        @pl.when((rel >= 2) & (lax.rem(rel, 2) == 0))
        def _():
            forward_copy(rel).start()

        part[...] = lax.dot_general(
            density_ref[...], eig[rel], (((1,), (1,)), ((), ())),
            preferred_element_type=jnp.float32,
        ).reshape(part.shape)
        sent[rel] = part[...].astype(jnp.bfloat16)
        own[rel] = part[z]
        for k in (2, 1, 3):
            red_copy(rel, k).start()

    def reduce(rel):
        for k in range(1, n_z):
            red_copy(rel, k).wait_recv()
        total = own[rel]
        for k in range(1, n_z):
            total = total + landed[rel, k - 1].astype(jnp.float32)
        proj[rel, z] = (total * keep_ref[z]).astype(jnp.bfloat16)
        pass_on(rel, 0)

    def screen_step(rel):
        take(rel, n_z - 2)
        whole = proj[rel].reshape(n_z * rows, depth)
        at = flip(band, rel)
        for half in range(2):
            acc[half] += lax.dot_general(
                whole, screen[at, half * depth : (half + 1) * depth], (((1,), (1,)), ((), ())),
                preferred_element_type=jnp.float32,
            )

    def step(t, carry):
        @pl.when(t < n_rel)
        def _():
            project(t)

        @pl.when((t >= 1) & (t < n_rel + 1))
        def _():
            reduce(t - 1)

        for hop in range(n_z - 2):
            @pl.when((t >= 2 + hop) & (t < n_rel + 2 + hop))
            def _():
                take(t - 2 - hop, hop)
                pass_on(t - 2 - hop, hop + 1)

        @pl.when(t >= n_z)
        def _():
            screen_step(t - n_z)

        return carry

    lax.fori_loop(0, n_rel + n_z, step, 0)

    screened = acc[...].astype(jnp.bfloat16)
    pairs = [proj[flip(band, 2 * z + half)].reshape(n_z * rows, depth) for half in range(2)]
    for slot in range(slots):
        here = slice(slot * block, (slot + 1) * block)
        total = 0.0
        for half in range(2):
            total = total + lax.dot_general(
                screened[half, here], pairs[half][here], (((1,), (1,)), ((), ())),
                preferred_element_type=jnp.float32,
            )
        total = total * weight_ref[slot]
        bands = lax.broadcasted_iota(jnp.int32, (place.shape[0], block), 0)
        window = start_ref[slot] + lax.broadcasted_iota(jnp.int32, (place.shape[0], block), 1)
        onehot = jnp.where(bands == window, 1.0, 0.0).astype(jnp.bfloat16)
        place[:, here] = onehot
        spread = 0.0
        for piece in split(total):
            spread = spread + jnp.dot(onehot, piece, preferred_element_type=jnp.float32)
        high[:, here], low[:, here] = split(spread)

    whole = 0.0
    for piece in (high, low):
        whole = whole + lax.dot_general(
            piece[...], place[...], (((1,), (1,)), ((), ())), preferred_element_type=jnp.float32
        )
    sigma[...] = whole.reshape(sigma.shape)

    def sigma_copy(rel):
        target = flip(band, rel)
        return pltpu.make_async_remote_copy(
            src_ref=sigma.at[target], dst_ref=sigma_in.at[rel - 1],
            send_sem=sig_send.at[rel - 1], recv_sem=sig_recv.at[rel - 1],
            device_id=(target, z), device_id_type=mesh_id,
        )

    def final_copy(k):
        target = lax.rem(z + k, n_z)
        return pltpu.make_async_remote_copy(
            src_ref=band_sum.at[target], dst_ref=band_in.at[k - 1],
            send_sem=fin_send.at[k - 1], recv_sem=fin_recv.at[k - 1],
            device_id=(band, target), device_id_type=mesh_id,
        )

    for rel in (6, 7, 2, 4, 3, 5, 1):
        sigma_copy(rel).start()
    total = sigma[band]
    for rel in range(1, n_rel):
        sigma_copy(rel).wait_recv()
        total = total + sigma_in[rel - 1]
    band_sum[...] = total.reshape(band_sum.shape)
    for k in (2, 1, 3):
        final_copy(k).start()
    total = band_sum[z]
    for k in range(1, n_z):
        final_copy(k).wait_recv()
        total = total + band_in[k - 1]
    out_ref[...] = total

    for rel in range(1, n_rel):
        sigma_copy(rel).wait_send()
    for k in range(1, n_z):
        final_copy(k).wait_send()

    for rel in (1, 2, 4, 6):
        eig_copy(rel).wait_send()
    for rel in (2, 4, 6):
        forward_copy(rel).wait_send()

    def drain(rel, carry):
        for k in range(1, n_z):
            red_copy(rel, k).wait_send()
        for hop in range(n_z - 1):
            @pl.when((z - hop >= 0) & (z + 1 < n_z))
            def _():
                up_copy(rel, hop).wait_send()

            @pl.when((z + hop < n_z) & (z >= 1))
            def _():
                down_copy(rel, hop).wait_send()
        return carry

    lax.fori_loop(0, n_rel, drain, 0)


def per_device(
    n_z, n_rel, pair_density, eigvecs, screening, occupation, window_start, window_len, slot_band
):
    slots, block, plane_rows = pair_density.shape
    depth, width = eigvecs.shape[0], screening.shape[0]
    rows = slots * block // n_z
    keep_rows = (
        (jnp.arange(block, dtype=jnp.int32)[None, :] < window_len[:, None])
        & (slot_band[:, None] >= 0)
    ).astype(jnp.float32)
    band_list = jnp.arange(occupation.shape[0], dtype=jnp.int32)
    weights = 0.5 - jnp.sum(
        jnp.where(band_list[None, :] == slot_band[:, None], occupation[None, :], 0.0), axis=1
    )
    dma = pltpu.SemaphoreType.DMA
    vmem = pl.BlockSpec(memory_space=pltpu.VMEM)
    strip = NB_SIGMA // (n_rel * n_z)
    return pl.pallas_call(
        fused_kernel,
        out_shape=jax.ShapeDtypeStruct((strip, NB_SIGMA), jnp.float32),
        in_specs=[
            vmem, pl.BlockSpec(memory_space=pl.ANY), vmem, vmem, vmem,
            pl.BlockSpec(memory_space=pltpu.SMEM),
        ],
        out_specs=vmem,
        scratch_shapes=[
            pltpu.VMEM((n_rel, depth, plane_rows), jnp.bfloat16),
            pltpu.VMEM((n_rel, width, depth), jnp.bfloat16),
            pltpu.VMEM((n_z, rows, depth), jnp.float32),
            pltpu.VMEM((n_rel, n_z, rows, depth), jnp.bfloat16),
            pltpu.VMEM((n_rel, rows, depth), jnp.float32),
            pltpu.VMEM((n_rel, n_z - 1, rows, depth), jnp.bfloat16),
            pltpu.VMEM((n_rel, n_z, rows, depth), jnp.bfloat16),
            pltpu.VMEM((2, slots * block, depth), jnp.float32),
            pltpu.VMEM((NB_SIGMA, slots * block), jnp.bfloat16),
            pltpu.VMEM((NB_SIGMA, slots * block), jnp.bfloat16),
            pltpu.VMEM((NB_SIGMA, slots * block), jnp.bfloat16),
            pltpu.VMEM((n_rel, n_z * strip, NB_SIGMA), jnp.float32),
            pltpu.VMEM((n_z, strip, NB_SIGMA), jnp.float32),
            pltpu.VMEM((n_rel - 1, n_z * strip, NB_SIGMA), jnp.float32),
            pltpu.VMEM((n_z - 1, strip, NB_SIGMA), jnp.float32),
            dma,
            dma((n_rel,)),
            dma((n_rel,)),
            dma((n_rel, n_z - 1)),
            dma((n_rel, n_z - 1)),
            dma((n_rel, n_z - 1)),
            dma((n_rel, n_z - 1)),
            dma((n_rel, n_z - 1)),
            dma((n_rel, n_z - 1)),
            dma((n_rel - 1,)),
            dma((n_rel - 1,)),
            dma((n_z - 1,)),
            dma((n_z - 1,)),
        ],
        compiler_params=pltpu.CompilerParams(
            collective_id=0, has_side_effects=True, vmem_limit_bytes=60 * 2**20
        ),
    )(
        pair_density.reshape(slots * block, plane_rows),
        eigvecs,
        screening,
        keep_rows.reshape(n_z, rows, 1),
        jnp.broadcast_to(weights[:, None, None], (slots, 8, block))[:, :1],
        window_start,
    )


def solution(mesh):
    n_band, n_z = mesh.shape["band"], mesh.shape["pw"]
    body = ring_per_device
    if n_band == 8 and n_z == 4:
        body = functools.partial(per_device, n_z, n_band)
    return jax.shard_map(
        body,
        mesh=mesh,
        in_specs=(
            P("band", None, "pw"),
            P("band", "pw"),
            P("pw", None),
            P(),
            P("band"),
            P("band"),
            P("band"),
        ),
        out_specs=P(("band", "pw"), None),
        check_vma=False,
    )
```

```python
import functools

import jax
import jax.numpy as jnp
from jax import lax
from jax.experimental import pallas as pl
from jax.experimental.pallas import tpu as pltpu
from jax.sharding import PartitionSpec as P

NB_SIGMA = 512


def ring_per_device(pair_density, eigvecs, screening, occupation, window_start, window_len, slot_band):
    capacity, block, plane_rows = pair_density.shape
    density, starts, lengths, band_ids = (pair_density, window_start, window_len, slot_band)
    slots = density.shape[0]
    flat = density.reshape(slots * block, plane_rows)
    partial_proj = lax.dot_general(
        flat,
        lax.all_gather(eigvecs, "band", axis=0, tiled=True),
        (((1,), (1,)), ((), ())),
        preferred_element_type=jnp.float32,
    )
    row_ids = jnp.arange(block, dtype=jnp.int32)
    keep_rows = ((row_ids[None, :] < lengths[:, None]) & (band_ids[:, None] >= 0)).astype(
        jnp.float32
    )
    masked = partial_proj * keep_rows.reshape(slots * block, 1)
    projected = lax.psum(masked, "pw").astype(jnp.bfloat16)
    width = screening.shape[0]
    own_cols = lax.dynamic_slice_in_dim(projected, lax.axis_index("pw") * width, width, 1)
    screened = lax.dot_general(
        projected, screening, (((1,), (1,)), ((), ())), preferred_element_type=jnp.float32
    ).astype(jnp.bfloat16)
    block_sigma = lax.dot_general(
        screened.reshape(slots, block, width),
        own_cols.reshape(slots, block, width),
        (((2,), (2,)), ((0,), (0,))),
        preferred_element_type=jnp.float32,
    )
    band_list = jnp.arange(occupation.shape[0], dtype=jnp.int32)
    weights = 0.5 - jnp.sum(
        jnp.where(band_list[None, :] == band_ids[:, None], occupation[None, :], 0.0), axis=1
    )
    totals = jnp.zeros((NB_SIGMA + block, NB_SIGMA + block), jnp.float32)
    for index in range(slots):
        first = starts[index]
        previous = lax.dynamic_slice(totals, (first, first), (block, block))
        totals = lax.dynamic_update_slice(
            totals, previous + weights[index] * block_sigma[index], (first, first)
        )
    sigma_part = totals[:NB_SIGMA, :NB_SIGMA]
    by_band = lax.psum_scatter(sigma_part, "band", scatter_dimension=0, tiled=True)
    return lax.psum_scatter(by_band, "pw", scatter_dimension=0, tiled=True)


def flip(index, relation):
    total = 0
    for place in (4, 2, 1):
        bit = lax.rem(index // place, 2)
        other = lax.rem(relation // place, 2)
        total = total + place * (bit + other - 2 * bit * other)
    return total


def split(value):
    top = value.astype(jnp.bfloat16)
    return top, (value - top.astype(jnp.float32)).astype(jnp.bfloat16)


def fused_kernel(
    density_ref, eig_ref, screen_ref, meta_ref, out_ref,
    density, extra, extra_meta, meta, eig, screen, part, sent, own, landed, proj, acc,
    place, high, low, sigma, band_sum, sigma_in, band_in,
    load_sem, extra_send, extra_recv, eig_send, eig_recv, red_send, red_recv, up_send, up_recv, down_send, down_recv,
    sig_send, sig_recv, fin_send, fin_recv,
):
    mesh_id = pl.DeviceIdType.MESH
    band, z = lax.axis_index("band"), lax.axis_index("pw")
    n_rel, depth, _ = eig.shape
    n_z = landed.shape[1] + 1
    rows = own.shape[1]
    slots, block = n_z, rows
    last = slots * block

    barrier = pltpu.get_barrier_semaphore()
    for rel in range(1, n_rel):
        pl.semaphore_signal(barrier, inc=1, device_id=(flip(band, rel), z), device_id_type=mesh_id)
    for k in range(1, n_z):
        pl.semaphore_signal(
            barrier, inc=1, device_id=(band, lax.rem(z + k, n_z)), device_id_type=mesh_id
        )
    loads = [
        pltpu.make_async_copy(density_ref.at[pl.ds(0, last)], density, load_sem.at[0]),
        pltpu.make_async_copy(eig_ref, eig.at[0], load_sem.at[1]),
    ]
    for load in loads:
        load.start()
    pl.semaphore_wait(barrier, n_rel - 1 + n_z - 1)

    def eig_copy(rel):
        return pltpu.make_async_remote_copy(
            src_ref=eig_ref, dst_ref=eig.at[rel], send_sem=eig_send.at[rel],
            recv_sem=eig_recv.at[rel], device_id=(flip(band, rel), z), device_id_type=mesh_id,
        )

    def forward_copy(rel):
        return pltpu.make_async_remote_copy(
            src_ref=eig.at[rel], dst_ref=eig.at[rel + 1], send_sem=eig_send.at[rel + 1],
            recv_sem=eig_recv.at[rel + 1], device_id=(flip(band, 1), z), device_id_type=mesh_id,
        )

    partner = (flip(band, n_rel // 2), z)
    swaps = [
        pltpu.make_async_remote_copy(
            src_ref=source, dst_ref=target, send_sem=extra_send.at[index],
            recv_sem=extra_recv.at[index], device_id=partner, device_id_type=mesh_id,
        )
        for index, (source, target) in enumerate(
            [(density_ref.at[pl.ds(last, block)], extra), (meta_ref.at[slots], extra_meta)]
        )
    ]
    for swap in swaps:
        swap.start()
    for rel in (1, 2, 4, 6):
        eig_copy(rel).start()
    def red_copy(rel, k):
        target = lax.rem(z + k, n_z)
        return pltpu.make_async_remote_copy(
            src_ref=sent.at[rel, target], dst_ref=landed.at[rel, k - 1],
            send_sem=red_send.at[rel, k - 1], recv_sem=red_recv.at[rel, k - 1],
            device_id=(band, target), device_id_type=mesh_id,
        )

    def up_copy(rel, hop):
        source = lax.rem(z - hop + n_z, n_z)
        return pltpu.make_async_remote_copy(
            src_ref=proj.at[rel, source], dst_ref=proj.at[rel, source],
            send_sem=up_send.at[rel, hop], recv_sem=up_recv.at[rel, hop],
            device_id=(band, lax.rem(z + 1, n_z)), device_id_type=mesh_id,
        )

    def down_copy(rel, hop):
        source = lax.rem(z + hop, n_z)
        return pltpu.make_async_remote_copy(
            src_ref=proj.at[rel, source], dst_ref=proj.at[rel, source],
            send_sem=down_send.at[rel, hop], recv_sem=down_recv.at[rel, hop],
            device_id=(band, lax.rem(z + n_z - 1, n_z)), device_id_type=mesh_id,
        )

    def landing(rel, hop, up):
        source = lax.rem(z - hop - 1 + 2 * n_z, n_z) if up else lax.rem(z + hop + 1, n_z)
        return pltpu.make_async_remote_copy(
            src_ref=proj.at[rel, source], dst_ref=proj.at[rel, source],
            send_sem=(up_send if up else down_send).at[rel, hop],
            recv_sem=(up_recv if up else down_recv).at[rel, hop],
            device_id=(band, lax.rem(z + 1, n_z)), device_id_type=mesh_id,
        )

    def pass_on(rel, hop):
        @pl.when((z - hop >= 0) & (z + 1 < n_z))
        def _():
            up_copy(rel, hop).start()

        @pl.when((z + hop < n_z) & (z >= 1))
        def _():
            down_copy(rel, hop).start()

    def take(rel, hop):
        @pl.when(z - hop - 1 >= 0)
        def _():
            landing(rel, hop, True).wait_recv()

        @pl.when(z + hop + 1 < n_z)
        def _():
            landing(rel, hop, False).wait_recv()

    def multiply(rel, first, stop):
        result = lax.dot_general(
            density[first * block : stop * block], eig[rel], (((1,), (1,)), ((), ())),
            preferred_element_type=jnp.float32,
        ).reshape(stop - first, block, depth)
        part[first:stop] = result
        sent[rel, first:stop] = result.astype(jnp.bfloat16)

        @pl.when((z >= first) & (z < stop))
        def _():
            own[rel] = part[z]

        for k in (2, 1, 3):
            target = lax.rem(z + k, n_z)

            @pl.when((target >= first) & (target < stop))
            def _():
                red_copy(rel, k).start()

    def project(rel):
        @pl.when(rel >= 1)
        def _():
            eig_copy(rel).wait_recv()

        @pl.when((rel >= 2) & (lax.rem(rel, 2) == 0))
        def _():
            forward_copy(rel).start()

        @pl.when(rel == 0)
        def _():
            for swap in swaps:
                swap.wait_recv()
            taken = meta_ref[slots - 1, 0:1, 0:1] > 0.0
            for slot in range(slots - 1):
                meta[slot] = meta_ref[slot]
            meta[slots - 1] = jnp.where(taken, meta_ref[slots - 1], extra_meta[...])
            tail = density[last - block :]
            density[last - block :] = jnp.where(taken, tail, extra[...])
            multiply(rel, slots - 1, slots)

        @pl.when(rel > 0)
        def _():
            multiply(rel, 0, slots)

    def reduce(rel):
        for k in range(1, n_z):
            red_copy(rel, k).wait_recv()
        total = own[rel]
        for k in range(1, n_z):
            total = total + landed[rel, k - 1].astype(jnp.float32)
        row_ids = lax.broadcasted_iota(jnp.int32, total.shape, 0).astype(jnp.float32)
        keep = jnp.where(row_ids < meta[z, 0:1, 0:1], 1.0, 0.0)
        proj[rel, z] = (total * keep).astype(jnp.bfloat16)
        pass_on(rel, 0)

    def screen_step(rel):
        take(rel, n_z - 2)
        whole = proj[rel].reshape(n_z * rows, depth)
        at = flip(band, rel)
        for half in range(2):
            acc[half] += lax.dot_general(
                whole, screen[at, half * depth : (half + 1) * depth], (((1,), (1,)), ((), ())),
                preferred_element_type=jnp.float32,
            )

    def step(t, carry):
        @pl.when(t < n_rel)
        def _():
            project(t)

        @pl.when((t >= 1) & (t < n_rel + 1))
        def _():
            reduce(t - 1)

        for hop in range(n_z - 2):
            @pl.when((t >= 2 + hop) & (t < n_rel + 2 + hop))
            def _():
                take(t - 2 - hop, hop)
                pass_on(t - 2 - hop, hop + 1)

        @pl.when(t >= n_z)
        def _():
            screen_step(t - n_z)

        return carry

    for load in loads:
        load.wait()
    multiply(0, 0, slots - 1)
    for index in range(n_rel):
        screen[index] = screen_ref[:, index * depth : (index + 1) * depth]
    acc[...] = jnp.zeros_like(acc)
    lax.fori_loop(0, n_rel + n_z, step, 0)

    screened = acc[...].astype(jnp.bfloat16)
    pairs = [proj[flip(band, 2 * z + half)].reshape(n_z * rows, depth) for half in range(2)]
    for slot in range(slots):
        here = slice(slot * block, (slot + 1) * block)
        total = 0.0
        for half in range(2):
            total = total + lax.dot_general(
                screened[half, here], pairs[half][here], (((1,), (1,)), ((), ())),
                preferred_element_type=jnp.float32,
            )
        total = total * meta[slot, 1:2]
        bands = lax.broadcasted_iota(jnp.int32, (place.shape[0], block), 0).astype(jnp.float32)
        window = lax.broadcasted_iota(jnp.int32, (place.shape[0], block), 1).astype(jnp.float32)
        window = window + meta[slot, 2:3]
        onehot = jnp.where(bands == window, 1.0, 0.0).astype(jnp.bfloat16)
        place[:, here] = onehot
        spread = 0.0
        for piece in split(total):
            spread = spread + jnp.dot(onehot, piece, preferred_element_type=jnp.float32)
        high[:, here], low[:, here] = split(spread)

    whole = 0.0
    for piece in (high, low):
        whole = whole + lax.dot_general(
            piece[...], place[...], (((1,), (1,)), ((), ())), preferred_element_type=jnp.float32
        )
    sigma[...] = whole.reshape(sigma.shape)

    def sigma_copy(rel):
        target = flip(band, rel)
        return pltpu.make_async_remote_copy(
            src_ref=sigma.at[target], dst_ref=sigma_in.at[rel - 1],
            send_sem=sig_send.at[rel - 1], recv_sem=sig_recv.at[rel - 1],
            device_id=(target, z), device_id_type=mesh_id,
        )

    def final_copy(k):
        target = lax.rem(z + k, n_z)
        return pltpu.make_async_remote_copy(
            src_ref=band_sum.at[target], dst_ref=band_in.at[k - 1],
            send_sem=fin_send.at[k - 1], recv_sem=fin_recv.at[k - 1],
            device_id=(band, target), device_id_type=mesh_id,
        )

    for rel in (6, 7, 2, 4, 3, 5, 1):
        sigma_copy(rel).start()
    total = sigma[band]
    for rel in range(1, n_rel):
        sigma_copy(rel).wait_recv()
        total = total + sigma_in[rel - 1]
    band_sum[...] = total.reshape(band_sum.shape)
    for k in (2, 1, 3):
        final_copy(k).start()
    total = band_sum[z]
    for k in range(1, n_z):
        final_copy(k).wait_recv()
        total = total + band_in[k - 1]
    out_ref[...] = total

    for rel in range(1, n_rel):
        sigma_copy(rel).wait_send()
    for k in range(1, n_z):
        final_copy(k).wait_send()

    for swap in swaps:
        swap.wait_send()
    for rel in (1, 2, 4, 6):
        eig_copy(rel).wait_send()
    for rel in (2, 4, 6):
        forward_copy(rel).wait_send()

    def drain(rel, carry):
        for k in range(1, n_z):
            red_copy(rel, k).wait_send()
        for hop in range(n_z - 1):
            @pl.when((z - hop >= 0) & (z + 1 < n_z))
            def _():
                up_copy(rel, hop).wait_send()

            @pl.when((z + hop < n_z) & (z >= 1))
            def _():
                down_copy(rel, hop).wait_send()
        return carry

    lax.fori_loop(0, n_rel, drain, 0)


def per_device(
    n_z, n_rel, pair_density, eigvecs, screening, occupation, window_start, window_len, slot_band
):
    capacity, block, plane_rows = pair_density.shape
    depth, width = eigvecs.shape[0], screening.shape[0]
    slots, rows = n_z, block
    kept = jnp.where(slot_band >= 0, window_len, 0).astype(jnp.float32)
    band_list = jnp.arange(occupation.shape[0], dtype=jnp.int32)
    weights = 0.5 - jnp.sum(
        jnp.where(band_list[None, :] == slot_band[:, None], occupation[None, :], 0.0), axis=1
    )
    fields = jnp.stack([kept, weights, window_start.astype(jnp.float32)], axis=1)
    meta = jnp.broadcast_to(jnp.pad(fields, ((0, 0), (0, 5)))[:, :, None], (capacity, 8, block))
    dma = pltpu.SemaphoreType.DMA
    vmem = pl.BlockSpec(memory_space=pltpu.VMEM)
    strip = NB_SIGMA // (n_rel * n_z)
    return pl.pallas_call(
        fused_kernel,
        out_shape=jax.ShapeDtypeStruct((strip, NB_SIGMA), jnp.float32),
        in_specs=[
            pl.BlockSpec(memory_space=pl.ANY), pl.BlockSpec(memory_space=pl.ANY), vmem, vmem,
        ],
        out_specs=vmem,
        scratch_shapes=[
            pltpu.VMEM((slots * block, plane_rows), jnp.bfloat16),
            pltpu.VMEM((block, plane_rows), jnp.bfloat16),
            pltpu.VMEM((8, block), jnp.float32),
            pltpu.VMEM((slots, 8, block), jnp.float32),
            pltpu.VMEM((n_rel, depth, plane_rows), jnp.bfloat16),
            pltpu.VMEM((n_rel, width, depth), jnp.bfloat16),
            pltpu.VMEM((n_z, rows, depth), jnp.float32),
            pltpu.VMEM((n_rel, n_z, rows, depth), jnp.bfloat16),
            pltpu.VMEM((n_rel, rows, depth), jnp.float32),
            pltpu.VMEM((n_rel, n_z - 1, rows, depth), jnp.bfloat16),
            pltpu.VMEM((n_rel, n_z, rows, depth), jnp.bfloat16),
            pltpu.VMEM((2, slots * block, depth), jnp.float32),
            pltpu.VMEM((NB_SIGMA, slots * block), jnp.bfloat16),
            pltpu.VMEM((NB_SIGMA, slots * block), jnp.bfloat16),
            pltpu.VMEM((NB_SIGMA, slots * block), jnp.bfloat16),
            pltpu.VMEM((n_rel, n_z * strip, NB_SIGMA), jnp.float32),
            pltpu.VMEM((n_z, strip, NB_SIGMA), jnp.float32),
            pltpu.VMEM((n_rel - 1, n_z * strip, NB_SIGMA), jnp.float32),
            pltpu.VMEM((n_z - 1, strip, NB_SIGMA), jnp.float32),
            dma((2,)),
            dma((2,)),
            dma((2,)),
            dma((n_rel,)),
            dma((n_rel,)),
            dma((n_rel, n_z - 1)),
            dma((n_rel, n_z - 1)),
            dma((n_rel, n_z - 1)),
            dma((n_rel, n_z - 1)),
            dma((n_rel, n_z - 1)),
            dma((n_rel, n_z - 1)),
            dma((n_rel - 1,)),
            dma((n_rel - 1,)),
            dma((n_z - 1,)),
            dma((n_z - 1,)),
        ],
        compiler_params=pltpu.CompilerParams(
            collective_id=0, has_side_effects=True, vmem_limit_bytes=60 * 2**20
        ),
    )(
        pair_density.reshape(capacity * block, plane_rows),
        eigvecs,
        screening,
        meta,
    )


def solution(mesh):
    n_band, n_z = mesh.shape["band"], mesh.shape["pw"]
    body = ring_per_device
    if n_band == 8 and n_z == 4:
        body = functools.partial(per_device, n_z, n_band)
    return jax.shard_map(
        body,
        mesh=mesh,
        in_specs=(
            P("band", None, "pw"),
            P("band", "pw"),
            P("pw", None),
            P(),
            P("band"),
            P("band"),
            P("band"),
        ),
        out_specs=P(("band", "pw"), None),
        check_vma=False,
    )
```

```python
import functools

import jax
import jax.numpy as jnp
from jax import lax
from jax.experimental import pallas as pl
from jax.experimental.pallas import tpu as pltpu
from jax.sharding import PartitionSpec as P

NB_SIGMA = 512


def ring_per_device(pair_density, eigvecs, screening, occupation, window_start, window_len, slot_band):
    capacity, block, plane_rows = pair_density.shape
    density, starts, lengths, band_ids = (pair_density, window_start, window_len, slot_band)
    slots = density.shape[0]
    flat = density.reshape(slots * block, plane_rows)
    partial_proj = lax.dot_general(
        flat,
        lax.all_gather(eigvecs, "band", axis=0, tiled=True),
        (((1,), (1,)), ((), ())),
        preferred_element_type=jnp.float32,
    )
    row_ids = jnp.arange(block, dtype=jnp.int32)
    keep_rows = ((row_ids[None, :] < lengths[:, None]) & (band_ids[:, None] >= 0)).astype(
        jnp.float32
    )
    masked = partial_proj * keep_rows.reshape(slots * block, 1)
    projected = lax.psum(masked, "pw").astype(jnp.bfloat16)
    width = screening.shape[0]
    own_cols = lax.dynamic_slice_in_dim(projected, lax.axis_index("pw") * width, width, 1)
    screened = lax.dot_general(
        projected, screening, (((1,), (1,)), ((), ())), preferred_element_type=jnp.float32
    ).astype(jnp.bfloat16)
    block_sigma = lax.dot_general(
        screened.reshape(slots, block, width),
        own_cols.reshape(slots, block, width),
        (((2,), (2,)), ((0,), (0,))),
        preferred_element_type=jnp.float32,
    )
    band_list = jnp.arange(occupation.shape[0], dtype=jnp.int32)
    weights = 0.5 - jnp.sum(
        jnp.where(band_list[None, :] == band_ids[:, None], occupation[None, :], 0.0), axis=1
    )
    totals = jnp.zeros((NB_SIGMA + block, NB_SIGMA + block), jnp.float32)
    for index in range(slots):
        first = starts[index]
        previous = lax.dynamic_slice(totals, (first, first), (block, block))
        totals = lax.dynamic_update_slice(
            totals, previous + weights[index] * block_sigma[index], (first, first)
        )
    sigma_part = totals[:NB_SIGMA, :NB_SIGMA]
    by_band = lax.psum_scatter(sigma_part, "band", scatter_dimension=0, tiled=True)
    return lax.psum_scatter(by_band, "pw", scatter_dimension=0, tiled=True)


def flip(index, relation):
    total = 0
    for place in (4, 2, 1):
        bit = lax.rem(index // place, 2)
        other = lax.rem(relation // place, 2)
        total = total + place * (bit + other - 2 * bit * other)
    return total


def split(value):
    top = value.astype(jnp.bfloat16)
    return top, (value - top.astype(jnp.float32)).astype(jnp.bfloat16)


def fused_kernel(
    density_ref, eig_ref, screen_ref, meta_ref, out_ref,
    density, extra, extra_meta, meta, eig, screen, part, sent, own, landed, proj, acc,
    place, high, low, sigma, band_sum, sigma_in, band_in,
    load_sem, extra_send, extra_recv, half_send, half_recv, eig_send, eig_recv, red_send, red_recv, up_send, up_recv, down_send, down_recv,
    sig_send, sig_recv, fin_send, fin_recv,
):
    mesh_id = pl.DeviceIdType.MESH
    band, z = lax.axis_index("band"), lax.axis_index("pw")
    n_rel, depth, _ = eig.shape
    n_z = landed.shape[1] + 1
    rows = own.shape[1]
    slots, block = n_z, rows
    last = slots * block

    barrier = pltpu.get_barrier_semaphore()
    for rel in range(1, n_rel):
        pl.semaphore_signal(barrier, inc=1, device_id=(flip(band, rel), z), device_id_type=mesh_id)
    for k in range(1, n_z):
        pl.semaphore_signal(
            barrier, inc=1, device_id=(band, lax.rem(z + k, n_z)), device_id_type=mesh_id
        )
    loads = [
        pltpu.make_async_copy(density_ref.at[pl.ds(0, last)], density, load_sem.at[0]),
        pltpu.make_async_copy(eig_ref, eig.at[0], load_sem.at[1]),
    ]
    for load in loads:
        load.start()
    pl.semaphore_wait(barrier, n_rel - 1 + n_z - 1)

    middle = -(-depth // 32) * 16
    halves = (pl.ds(0, middle), pl.ds(middle, depth - middle))

    def half_copy(rel, half):
        return pltpu.make_async_remote_copy(
            src_ref=eig_ref.at[halves[half]], dst_ref=eig.at[rel, halves[half]],
            send_sem=half_send.at[half, rel], recv_sem=half_recv.at[half, rel],
            device_id=(flip(band, rel), z), device_id_type=mesh_id,
        )

    def corner_copy(half):
        via = (2, 4)[half]
        return pltpu.make_async_remote_copy(
            src_ref=eig.at[via, halves[half]], dst_ref=eig.at[6, halves[half]],
            send_sem=half_send.at[half, 6], recv_sem=half_recv.at[half, 6],
            device_id=(flip(band, 6 - via), z), device_id_type=mesh_id,
        )

    def eig_copy(rel):
        return pltpu.make_async_remote_copy(
            src_ref=eig_ref, dst_ref=eig.at[rel], send_sem=eig_send.at[rel],
            recv_sem=eig_recv.at[rel], device_id=(flip(band, rel), z), device_id_type=mesh_id,
        )

    def forward_copy(rel):
        return pltpu.make_async_remote_copy(
            src_ref=eig.at[rel], dst_ref=eig.at[rel + 1], send_sem=eig_send.at[rel + 1],
            recv_sem=eig_recv.at[rel + 1], device_id=(flip(band, 1), z), device_id_type=mesh_id,
        )

    partner = (flip(band, n_rel // 2), z)
    swaps = [
        pltpu.make_async_remote_copy(
            src_ref=source, dst_ref=target, send_sem=extra_send.at[index],
            recv_sem=extra_recv.at[index], device_id=partner, device_id_type=mesh_id,
        )
        for index, (source, target) in enumerate(
            [(density_ref.at[pl.ds(last, block)], extra), (meta_ref.at[slots], extra_meta)]
        )
    ]
    for swap in swaps:
        swap.start()
    for rel, half in ((2, 0), (4, 1), (2, 1), (4, 0)):
        half_copy(rel, half).start()
    eig_copy(1).start()
    def red_copy(rel, k):
        target = lax.rem(z + k, n_z)
        return pltpu.make_async_remote_copy(
            src_ref=sent.at[rel, target], dst_ref=landed.at[rel, k - 1],
            send_sem=red_send.at[rel, k - 1], recv_sem=red_recv.at[rel, k - 1],
            device_id=(band, target), device_id_type=mesh_id,
        )

    def up_copy(rel, hop):
        source = lax.rem(z - hop + n_z, n_z)
        return pltpu.make_async_remote_copy(
            src_ref=proj.at[rel, source], dst_ref=proj.at[rel, source],
            send_sem=up_send.at[rel, hop], recv_sem=up_recv.at[rel, hop],
            device_id=(band, lax.rem(z + 1, n_z)), device_id_type=mesh_id,
        )

    def down_copy(rel, hop):
        source = lax.rem(z + hop, n_z)
        return pltpu.make_async_remote_copy(
            src_ref=proj.at[rel, source], dst_ref=proj.at[rel, source],
            send_sem=down_send.at[rel, hop], recv_sem=down_recv.at[rel, hop],
            device_id=(band, lax.rem(z + n_z - 1, n_z)), device_id_type=mesh_id,
        )

    def landing(rel, hop, up):
        source = lax.rem(z - hop - 1 + 2 * n_z, n_z) if up else lax.rem(z + hop + 1, n_z)
        return pltpu.make_async_remote_copy(
            src_ref=proj.at[rel, source], dst_ref=proj.at[rel, source],
            send_sem=(up_send if up else down_send).at[rel, hop],
            recv_sem=(up_recv if up else down_recv).at[rel, hop],
            device_id=(band, lax.rem(z + 1, n_z)), device_id_type=mesh_id,
        )

    def pass_on(rel, hop):
        @pl.when((z - hop >= 0) & (z + 1 < n_z))
        def _():
            up_copy(rel, hop).start()

        @pl.when((z + hop < n_z) & (z >= 1))
        def _():
            down_copy(rel, hop).start()

    def take(rel, hop):
        @pl.when(z - hop - 1 >= 0)
        def _():
            landing(rel, hop, True).wait_recv()

        @pl.when(z + hop + 1 < n_z)
        def _():
            landing(rel, hop, False).wait_recv()

    def multiply(rel, first, stop):
        result = lax.dot_general(
            density[first * block : stop * block], eig[rel], (((1,), (1,)), ((), ())),
            preferred_element_type=jnp.float32,
        ).reshape(stop - first, block, depth)
        part[first:stop] = result
        sent[rel, first:stop] = result.astype(jnp.bfloat16)

        @pl.when((z >= first) & (z < stop))
        def _():
            own[rel] = part[z]

        for k in (2, 1, 3):
            target = lax.rem(z + k, n_z)

            @pl.when((target >= first) & (target < stop))
            def _():
                red_copy(rel, k).start()

    def project(rel):
        @pl.when(lax.rem(rel, 2) == 1)
        def _():
            eig_copy(rel).wait_recv()

        @pl.when(rel == 2)
        def _():
            half_copy(2, 0).wait_recv()
            corner_copy(0).start()
            half_copy(4, 1).wait_recv()
            corner_copy(1).start()
            half_copy(2, 1).wait_recv()

        @pl.when(rel == 4)
        def _():
            half_copy(4, 0).wait_recv()

        @pl.when(rel == 6)
        def _():
            corner_copy(0).wait_recv()
            corner_copy(1).wait_recv()

        @pl.when((rel >= 2) & (lax.rem(rel, 2) == 0))
        def _():
            forward_copy(rel).start()

        @pl.when(rel == 0)
        def _():
            for swap in swaps:
                swap.wait_recv()
            taken = meta_ref[slots - 1, 0:1, 0:1] > 0.0
            for slot in range(slots - 1):
                meta[slot] = meta_ref[slot]
            meta[slots - 1] = jnp.where(taken, meta_ref[slots - 1], extra_meta[...])
            tail = density[last - block :]
            density[last - block :] = jnp.where(taken, tail, extra[...])
            multiply(rel, slots - 1, slots)

        @pl.when(rel > 0)
        def _():
            multiply(rel, 0, slots)

    def reduce(rel):
        for k in range(1, n_z):
            red_copy(rel, k).wait_recv()
        total = own[rel]
        for k in range(1, n_z):
            total = total + landed[rel, k - 1].astype(jnp.float32)
        row_ids = lax.broadcasted_iota(jnp.int32, total.shape, 0).astype(jnp.float32)
        keep = jnp.where(row_ids < meta[z, 0:1, 0:1], 1.0, 0.0)
        proj[rel, z] = (total * keep).astype(jnp.bfloat16)
        pass_on(rel, 0)

    def screen_step(rel):
        take(rel, n_z - 2)
        whole = proj[rel].reshape(n_z * rows, depth)
        at = flip(band, rel)
        for half in range(2):
            acc[half] += lax.dot_general(
                whole, screen[at, half * depth : (half + 1) * depth], (((1,), (1,)), ((), ())),
                preferred_element_type=jnp.float32,
            )

    def step(t, carry):
        @pl.when(t < n_rel)
        def _():
            project(t)

        @pl.when((t >= 1) & (t < n_rel + 1))
        def _():
            reduce(t - 1)

        for hop in range(n_z - 2):
            @pl.when((t >= 2 + hop) & (t < n_rel + 2 + hop))
            def _():
                take(t - 2 - hop, hop)
                pass_on(t - 2 - hop, hop + 1)

        @pl.when(t >= n_z)
        def _():
            screen_step(t - n_z)

        return carry

    for load in loads:
        load.wait()
    multiply(0, 0, slots - 1)
    for index in range(n_rel):
        screen[index] = screen_ref[:, index * depth : (index + 1) * depth]
    acc[...] = jnp.zeros_like(acc)
    lax.fori_loop(0, n_rel + n_z, step, 0)

    screened = acc[...].astype(jnp.bfloat16)
    pairs = [proj[flip(band, 2 * z + half)].reshape(n_z * rows, depth) for half in range(2)]
    for slot in range(slots):
        here = slice(slot * block, (slot + 1) * block)
        total = 0.0
        for half in range(2):
            total = total + lax.dot_general(
                screened[half, here], pairs[half][here], (((1,), (1,)), ((), ())),
                preferred_element_type=jnp.float32,
            )
        total = total * meta[slot, 1:2]
        bands = lax.broadcasted_iota(jnp.int32, (place.shape[0], block), 0).astype(jnp.float32)
        window = lax.broadcasted_iota(jnp.int32, (place.shape[0], block), 1).astype(jnp.float32)
        window = window + meta[slot, 2:3]
        onehot = jnp.where(bands == window, 1.0, 0.0).astype(jnp.bfloat16)
        place[:, here] = onehot
        spread = 0.0
        for piece in split(total):
            spread = spread + jnp.dot(onehot, piece, preferred_element_type=jnp.float32)
        high[:, here], low[:, here] = split(spread)

    whole = 0.0
    for piece in (high, low):
        whole = whole + lax.dot_general(
            piece[...], place[...], (((1,), (1,)), ((), ())), preferred_element_type=jnp.float32
        )
    sigma[...] = whole.reshape(sigma.shape)

    def sigma_copy(rel):
        target = flip(band, rel)
        return pltpu.make_async_remote_copy(
            src_ref=sigma.at[target], dst_ref=sigma_in.at[rel - 1],
            send_sem=sig_send.at[rel - 1], recv_sem=sig_recv.at[rel - 1],
            device_id=(target, z), device_id_type=mesh_id,
        )

    def final_copy(k):
        target = lax.rem(z + k, n_z)
        return pltpu.make_async_remote_copy(
            src_ref=band_sum.at[target], dst_ref=band_in.at[k - 1],
            send_sem=fin_send.at[k - 1], recv_sem=fin_recv.at[k - 1],
            device_id=(band, target), device_id_type=mesh_id,
        )

    for rel in (6, 7, 2, 4, 3, 5, 1):
        sigma_copy(rel).start()
    total = sigma[band]
    for rel in range(1, n_rel):
        sigma_copy(rel).wait_recv()
        total = total + sigma_in[rel - 1]
    band_sum[...] = total.reshape(band_sum.shape)
    for k in (2, 1, 3):
        final_copy(k).start()
    total = band_sum[z]
    for k in range(1, n_z):
        final_copy(k).wait_recv()
        total = total + band_in[k - 1]
    out_ref[...] = total

    for rel in range(1, n_rel):
        sigma_copy(rel).wait_send()
    for k in range(1, n_z):
        final_copy(k).wait_send()

    for swap in swaps:
        swap.wait_send()
    eig_copy(1).wait_send()
    for half in range(2):
        corner_copy(half).wait_send()
        for rel in (2, 4):
            half_copy(rel, half).wait_send()
    for rel in (2, 4, 6):
        forward_copy(rel).wait_send()

    def drain(rel, carry):
        for k in range(1, n_z):
            red_copy(rel, k).wait_send()
        for hop in range(n_z - 1):
            @pl.when((z - hop >= 0) & (z + 1 < n_z))
            def _():
                up_copy(rel, hop).wait_send()

            @pl.when((z + hop < n_z) & (z >= 1))
            def _():
                down_copy(rel, hop).wait_send()
        return carry

    lax.fori_loop(0, n_rel, drain, 0)


def per_device(
    n_z, n_rel, pair_density, eigvecs, screening, occupation, window_start, window_len, slot_band
):
    capacity, block, plane_rows = pair_density.shape
    depth, width = eigvecs.shape[0], screening.shape[0]
    slots, rows = n_z, block
    kept = jnp.where(slot_band >= 0, window_len, 0).astype(jnp.float32)
    band_list = jnp.arange(occupation.shape[0], dtype=jnp.int32)
    weights = 0.5 - jnp.sum(
        jnp.where(band_list[None, :] == slot_band[:, None], occupation[None, :], 0.0), axis=1
    )
    fields = jnp.stack([kept, weights, window_start.astype(jnp.float32)], axis=1)
    meta = jnp.broadcast_to(jnp.pad(fields, ((0, 0), (0, 5)))[:, :, None], (capacity, 8, block))
    dma = pltpu.SemaphoreType.DMA
    vmem = pl.BlockSpec(memory_space=pltpu.VMEM)
    strip = NB_SIGMA // (n_rel * n_z)
    return pl.pallas_call(
        fused_kernel,
        out_shape=jax.ShapeDtypeStruct((strip, NB_SIGMA), jnp.float32),
        in_specs=[
            pl.BlockSpec(memory_space=pl.ANY), pl.BlockSpec(memory_space=pl.ANY), vmem, vmem,
        ],
        out_specs=vmem,
        scratch_shapes=[
            pltpu.VMEM((slots * block, plane_rows), jnp.bfloat16),
            pltpu.VMEM((block, plane_rows), jnp.bfloat16),
            pltpu.VMEM((8, block), jnp.float32),
            pltpu.VMEM((slots, 8, block), jnp.float32),
            pltpu.VMEM((n_rel, depth, plane_rows), jnp.bfloat16),
            pltpu.VMEM((n_rel, width, depth), jnp.bfloat16),
            pltpu.VMEM((n_z, rows, depth), jnp.float32),
            pltpu.VMEM((n_rel, n_z, rows, depth), jnp.bfloat16),
            pltpu.VMEM((n_rel, rows, depth), jnp.float32),
            pltpu.VMEM((n_rel, n_z - 1, rows, depth), jnp.bfloat16),
            pltpu.VMEM((n_rel, n_z, rows, depth), jnp.bfloat16),
            pltpu.VMEM((2, slots * block, depth), jnp.float32),
            pltpu.VMEM((NB_SIGMA, slots * block), jnp.bfloat16),
            pltpu.VMEM((NB_SIGMA, slots * block), jnp.bfloat16),
            pltpu.VMEM((NB_SIGMA, slots * block), jnp.bfloat16),
            pltpu.VMEM((n_rel, n_z * strip, NB_SIGMA), jnp.float32),
            pltpu.VMEM((n_z, strip, NB_SIGMA), jnp.float32),
            pltpu.VMEM((n_rel - 1, n_z * strip, NB_SIGMA), jnp.float32),
            pltpu.VMEM((n_z - 1, strip, NB_SIGMA), jnp.float32),
            dma((2,)),
            dma((2,)),
            dma((2,)),
            dma((2, n_rel)),
            dma((2, n_rel)),
            dma((n_rel,)),
            dma((n_rel,)),
            dma((n_rel, n_z - 1)),
            dma((n_rel, n_z - 1)),
            dma((n_rel, n_z - 1)),
            dma((n_rel, n_z - 1)),
            dma((n_rel, n_z - 1)),
            dma((n_rel, n_z - 1)),
            dma((n_rel - 1,)),
            dma((n_rel - 1,)),
            dma((n_z - 1,)),
            dma((n_z - 1,)),
        ],
        compiler_params=pltpu.CompilerParams(
            collective_id=0, has_side_effects=True, vmem_limit_bytes=60 * 2**20
        ),
    )(
        pair_density.reshape(capacity * block, plane_rows),
        eigvecs,
        screening,
        meta,
    )


def solution(mesh):
    n_band, n_z = mesh.shape["band"], mesh.shape["pw"]
    body = ring_per_device
    if n_band == 8 and n_z == 4:
        body = functools.partial(per_device, n_z, n_band)
    return jax.shard_map(
        body,
        mesh=mesh,
        in_specs=(
            P("band", None, "pw"),
            P("band", "pw"),
            P("pw", None),
            P(),
            P("band"),
            P("band"),
            P("band"),
        ),
        out_specs=P(("band", "pw"), None),
        check_vma=False,
    )
```
